32 devices in a mesh: grp: 2 (over y), fib: 4 (over z), wav: 2 (over x), arm: 2 (over core).
Axes of the slice: x: 2, y: 2, z: 4, core: 2. Of those that a mesh axis runs over, the one named last changes fastest.
Arguments:
- spectra: bfloat16 [32, 2, 2, 128, 256], P(('grp', 'fib'), 'arm', None, None, 'wav'), parts along dimension 0, as said below
- bands: bfloat16 [32, 2, 11, 128, 256], P(('grp', 'fib'), 'arm', None, None, 'wav'), parts along dimension 0, may hold values from 0 to 0.29882812
- coverage: int32 [32, 128], P(('grp', 'fib')), parts along dimension 0, may hold values from 0 to 1, as said below
Outputs:
- flux_coadd: float32 [2, 256, 256], P('arm', ('grp', 'fib'), 'wav'), parts along dimension 1
- ivar_coadd: float32 [2, 256, 256], P('arm', ('grp', 'fib'), 'wav'), parts along dimension 1
- res_coadd: float32 [2, 11, 256, 256], P('arm', None, ('grp', 'fib'), 'wav'), parts along dimension 2
- model: float32 [2, 256, 256], P('arm', ('grp', 'fib'), 'wav'), parts along dimension 1
The draws below stay inside these ranges and needn't reach their ends.
There are 2 independent parts, one for each index of `grp`. The reference program is written for one: setup_inputs(seed, part) draws one part's arguments, and reference() takes and returns one part's arrays. A program takes and returns all parts, laid end to end along the dimension named above; each array names one. Nothing has to cross between parts.
Inputs may be any that keep to these rules, and one draw needn't show every extreme that they name: `spectra`: channel 1 (inverse variance) lies between 0.25 and 4. `coverage`: every fiber is observed by at least one exposure.
All inputs are finite; a program needn't handle non-finite values.
Results may differ from the reference program's by a relative error of at most 0.0003.
Values may be sent and summed in bfloat16 or wider, within the bound.
No kernel may reach another device: no remote copies, remote signals or barrier semaphores. Data moves between devices by JAX's collectives and lax.ppermute only.
A program may use at most 64 MiB of HBM per device.

```python
import math
import jax
import jax.numpy as jnp
from jax import lax

BANDS = 11
EXPOSURES = 16
FIBERS = 128
WAVES = 256
ARMS = 2


def draw_spectra(key, part):
    key_sig, key_noise, key_ivar, key_mean = jax.random.split(jax.random.fold_in(key, 11), 4)
    signal = jax.random.normal(key_sig, (1, ARMS, FIBERS, WAVES), jnp.float32)
    shape = (EXPOSURES, ARMS, FIBERS, WAVES)
    ivar = jnp.exp(jax.random.uniform(key_ivar, shape, jnp.float32, math.log(0.25), math.log(4.0)))
    noise = jax.random.normal(key_noise, shape, jnp.float32) * lax_rsqrt(ivar)
    flux = signal + noise
    return jnp.stack([flux, ivar], 2).astype(jnp.bfloat16)


def lax_rsqrt(values):
    return 1.0 / jnp.sqrt(values)


def draw_coverage(key, part):
    key_level, key_roll = jax.random.split(jax.random.fold_in(key, 7))
    level = jax.random.randint(key_level, (1, FIBERS), 1, 5)
    roll = jax.random.randint(key_roll, (EXPOSURES, FIBERS), 0, 4)
    expo = jnp.arange(EXPOSURES, dtype=jnp.int32)[:, None]
    fiber = jnp.arange(FIBERS, dtype=jnp.int32)[None, :]
    forced = expo == fiber % EXPOSURES
    return jnp.where((roll < level) | forced, 1, 0).astype(jnp.int32)


def steps_of(own_key, shape, cuts, smallest, top_value):
    loudness = 1.0
    for dim, parts in cuts:
        steps = jax.random.uniform(jax.random.fold_in(jax.random.fold_in(own_key, 6), dim), (parts,), jnp.float32, smallest / len(cuts), top_value / len(cuts))
        loudness = loudness * jnp.repeat(jnp.exp(steps), shape[dim] // parts).reshape((-1,) + (1,) * (len(shape) - 1 - dim))
    return loudness


def setup_inputs(seed: int = 0, part: int = 0) -> dict:
    keys = jax.random.split(jax.random.key(seed), 4)
    part_splits = jax.random.split(jax.random.fold_in(keys[3], part), 4)
    spectra = draw_spectra(jax.random.fold_in(jax.random.fold_in(keys[3], part), 71), part)
    bands = jnp.clip(0.29882812 * jax.random.uniform(part_splits[1], (EXPOSURES, ARMS, BANDS, FIBERS, WAVES), jnp.float32) ** steps_of(part_splits[1], (EXPOSURES, ARMS, BANDS, FIBERS, WAVES), ((0, 4), (1, 2), (4, 2)), -0.2, 0.2), 0.0, 0.29882812).astype(jnp.bfloat16)
    coverage = draw_coverage(jax.random.fold_in(jax.random.fold_in(keys[3], part), 71), part)
    return {"spectra": spectra, "bands": bands, "coverage": coverage}


def reference(spectra, bands, coverage):
    coverage_bf = coverage.astype(jnp.bfloat16)[:, None, :, None]
    weights = spectra[:, :, 1] * coverage_bf

    def accumulate(carry, items):
        weight_one, flux_one, band_one = items
        weight_one = weight_one.astype(jnp.float32)
        return (carry[0] + weight_one,
                carry[1] + weight_one * flux_one.astype(jnp.float32),
                carry[2] + weight_one[:, None] * band_one.astype(jnp.float32)), None

    arms, fibers, waves = weights.shape[1], weights.shape[2], weights.shape[3]
    nbands = bands.shape[2]
    start = (jnp.zeros((arms, fibers, waves), jnp.float32),
             jnp.zeros((arms, fibers, waves), jnp.float32),
             jnp.zeros((arms, nbands, fibers, waves), jnp.float32))
    (ivar_coadd, flux_sum, band_sum), _ = lax.scan(accumulate, start, (weights, spectra[:, :, 0], bands))
    flux_coadd = flux_sum / ivar_coadd
    res_coadd = band_sum / ivar_coadd[:, None]
    padded = jnp.pad(flux_coadd, ((0, 0), (0, 0), (5, 5)))
    model = res_coadd[:, 0] * padded[:, :, 0:waves]
    for band_idx in range(1, nbands):
        model = model + res_coadd[:, band_idx] * padded[:, :, band_idx:band_idx + waves]
    return flux_coadd, ivar_coadd, res_coadd, model
```

```python
import math

import jax
import jax.numpy as jnp
from jax import lax
from jax.experimental import pallas as pl
from jax.experimental.pallas import tpu as pltpu
from jax.sharding import PartitionSpec as P

HALO = 5
WEIGHT_MAX = 4.0
BAND_MAX = 0.2988282
HALF_MAX = 65000.0


def spectra_kernel(step_ref, spectra_ref, cover_ref, *outs):
    weight = spectra_ref[:, 0, 1].astype(jnp.float32) * cover_ref[...]
    flux = spectra_ref[:, 0, 0].astype(jnp.float32)
    pair = jnp.stack([jnp.sum(weight, 0), jnp.sum(weight * flux, 0)])
    step = pl.program_id(0)
    for slot, out in enumerate(outs):

        @pl.when(step == slot)
        def _():
            out[...] = pair


def bands_kernel(step_ref, spectra_ref, cover_ref, bands_ref, *outs):
    weight = spectra_ref[:, 0, 0].astype(jnp.float32) * cover_ref[...]
    step = pl.program_id(0)
    nbands = bands_ref.shape[2]
    for slot, out in enumerate(outs):

        @pl.when(step == slot)
        def _():
            for band in range(nbands):
                total = jnp.sum(weight * bands_ref[:, 0, band].astype(jnp.float32), 0)
                out[band] = total.astype(out.dtype)


def order_of(size):
    return sorted(range(1, size), key=lambda s: -min(s, size - s)) + [0]


def partial_sums(kernel, arrays, specs, shape, dtypes, targets, size):
    whole = pl.BlockSpec(shape, lambda g, t: (0,) * len(shape))
    return pl.pallas_call(
        kernel,
        out_shape=[jax.ShapeDtypeStruct(shape, d) for d in dtypes],
        grid_spec=pltpu.PrefetchScalarGridSpec(
            num_scalar_prefetch=1, grid=(size,), in_specs=specs, out_specs=[whole] * len(dtypes)
        ),
    )(targets, *arrays)


def local(spectra, bands, coverage):
    size = lax.axis_size("fib")
    exposures, _, nbands, fibers, width = bands.shape
    rows = fibers // size
    offsets = order_of(size)
    here = lax.axis_index("fib")
    targets = (here + jnp.array(offsets, jnp.int32)) % size
    cover = coverage.astype(jnp.float32)[:, :, None]
    cover_spec = pl.BlockSpec((exposures, rows, 1), lambda g, t: (0, t[g], 0))
    pairs = partial_sums(
        spectra_kernel,
        (spectra, cover),
        [pl.BlockSpec((exposures, 1, 2, rows, width), lambda g, t: (0, 0, 0, t[g], 0)), cover_spec],
        (2, rows, width),
        [jnp.float32] * size,
        targets,
        size,
    )
    sums = partial_sums(
        bands_kernel,
        (spectra, cover, bands),
        [
            pl.BlockSpec((exposures, 1, 1, rows, width), lambda g, t: (0, 0, 1, t[g], 0)),
            cover_spec,
            pl.BlockSpec((exposures, 1, nbands, rows, width), lambda g, t: (0, 0, 0, t[g], 0)),
        ],
        (nbands, rows, width),
        [jnp.float32] * size,
        targets,
        size,
    )

    def exchange(parts):
        return [
            lax.ppermute(part, "fib", [(i, (i + s) % size) for i in range(size)])
            for part, s in zip(parts, offsets[:-1])
        ]

    got_pairs = exchange(pairs[:-1])
    scale = 2.0 ** math.floor(math.log2(HALF_MAX / (exposures * WEIGHT_MAX * BAND_MAX)))
    got_sums = exchange([(s * scale).astype(jnp.float16) for s in sums[:-1]])
    pair = sum(got_pairs, pairs[-1])
    ivar = pair[0]
    flux = pair[1] / ivar
    before, after = halo(flux)
    padded = jnp.concatenate([before, flux, after], 1)
    total = sum([g.astype(jnp.float32) * (1 / scale) for g in got_sums], sums[-1])
    res = total / ivar
    model = sum(res[b] * padded[:, b : b + width] for b in range(nbands))
    return flux[None], ivar[None], res[None], model[None]


def halo(flux):
    size = lax.axis_size("wav")
    width = flux.shape[1]
    up = [(i, i + 1) for i in range(size - 1)]
    before = lax.ppermute(flux[:, width - HALO :], "wav", up)
    after = lax.ppermute(flux[:, :HALO], "wav", [(j, i) for i, j in up])
    return before, after


def solution(mesh):
    return jax.shard_map(
        local,
        mesh=mesh,
        in_specs=(
            P(("grp", "fib"), "arm", None, None, "wav"),
            P(("grp", "fib"), "arm", None, None, "wav"),
            P(("grp", "fib"), None),
        ),
        out_specs=(
            P("arm", ("grp", "fib"), "wav"),
            P("arm", ("grp", "fib"), "wav"),
            P("arm", None, ("grp", "fib"), "wav"),
            P("arm", ("grp", "fib"), "wav"),
        ),
        check_vma=False,
    )
```

```python
import math

import jax
import jax.numpy as jnp
from jax import lax
from jax.experimental import pallas as pl
from jax.experimental.pallas import tpu as pltpu
from jax.sharding import PartitionSpec as P

HALO = 5
WEIGHT_MAX = 4.0
BAND_MAX = 0.2988282
HALF_MAX = 65000.0


def order_of(size):
    return sorted(range(1, size), key=lambda s: -min(s, size - s)) + [0]


def sums_kernel(cover_ref, spectra_hbm, bands_hbm, *refs, offsets, scale):
    size = len(offsets)
    pairs, sums = refs[:size], refs[size : 2 * size]
    spectra, bands, weight, spectra_sem, bands_sem = refs[2 * size :]
    exposures, nbands, fibers, width = bands.shape
    rows = fibers // size
    here = lax.axis_index("fib")
    starts = [pl.multiple_of((here + s) % size * rows, rows) for s in offsets]
    copies = [pltpu.make_async_copy(spectra_hbm.at[:, 0], spectra, spectra_sem)]
    for slot, start in enumerate(starts):
        part = pl.ds(start, rows)
        copies.append(
            pltpu.make_async_copy(bands_hbm.at[:, 0, :, part], bands.at[:, :, part], bands_sem.at[slot])
        )
    for copy in copies:
        copy.start()
    cover = cover_ref[...].astype(jnp.float32)
    copies[0].wait()
    for e in range(exposures):
        column = jnp.broadcast_to(cover[e : e + 1], (width, fibers)).T
        weight[e] = spectra[e, 1].astype(jnp.float32) * column
    for slot, start in enumerate(starts):
        part = pl.ds(start, rows)
        part_weight = [weight[e, part] for e in range(exposures)]
        pairs[slot][0] = sum(part_weight[1:], part_weight[0])
        pairs[slot][1] = sum(part_weight[e] * spectra[e, 0, part].astype(jnp.float32) for e in range(exposures))
    for slot, start in enumerate(starts):
        part = pl.ds(start, rows)
        part_weight = [weight[e, part] for e in range(exposures)]
        copies[slot + 1].wait()
        for band in range(nbands):
            total = sum(part_weight[e] * bands[e, band, part].astype(jnp.float32) for e in range(exposures))
            sums[slot][band] = total * scale if slot < size - 1 else total


def partial_sums(spectra, bands, coverage, offsets, scale):
    size = len(offsets)
    exposures, _, nbands, fibers, width = bands.shape
    rows = fibers // size
    vmem = pl.BlockSpec(memory_space=pltpu.VMEM)
    hbm = pl.BlockSpec(memory_space=pl.ANY)
    shapes = [(2, rows, width)] * size + [(nbands, rows, width)] * size
    outs = pl.pallas_call(
        lambda *refs: sums_kernel(*refs, offsets=offsets, scale=scale),
        out_shape=[pltpu.VMEM(s, jnp.float32) for s in shapes],
        in_specs=[vmem, hbm, hbm],
        out_specs=[vmem] * (2 * size),
        scratch_shapes=[
            pltpu.VMEM((exposures, 2, fibers, width), jnp.bfloat16),
            pltpu.VMEM((exposures, nbands, fibers, width), jnp.bfloat16),
            pltpu.VMEM((exposures, fibers, width), jnp.float32),
            pltpu.SemaphoreType.DMA,
            pltpu.SemaphoreType.DMA((size,)),
        ],
        name="partial_sums",
    )(coverage, spectra, bands)
    return outs[:size], outs[size:]


def local(spectra, bands, coverage):
    size = lax.axis_size("fib")
    exposures, _, nbands, fibers, width = bands.shape
    offsets = order_of(size)
    scale = 2.0 ** math.floor(math.log2(HALF_MAX / (exposures * WEIGHT_MAX * BAND_MAX)))
    pairs, sums = partial_sums(spectra, bands, coverage, offsets, scale)

    def exchange(parts):
        return [
            lax.ppermute(part, "fib", [(i, (i + s) % size) for i in range(size)])
            for part, s in zip(parts, offsets[:-1])
        ]

    got_pairs = exchange(pairs[:-1])
    got_sums = exchange([s.astype(jnp.float16) for s in sums[:-1]])
    pair = sum(got_pairs, pairs[-1])
    ivar = pair[0]
    flux = pair[1] / ivar
    before, after = halo(flux)
    padded = jnp.concatenate([before, flux, after], 1)
    total = sum([g.astype(jnp.float32) * (1 / scale) for g in got_sums], sums[-1])
    res = total / ivar
    model = sum(res[b] * padded[:, b : b + width] for b in range(nbands))
    return flux[None], ivar[None], res[None], model[None]


def halo(flux):
    size = lax.axis_size("wav")
    width = flux.shape[1]
    first, last = flux[:, :HALO], flux[:, width - HALO :]
    if size == 2:
        low = lax.axis_index("wav") == 0
        got = lax.ppermute(jnp.where(low, last, first), "wav", [(0, 1), (1, 0)])
        return jnp.where(low, 0.0, got), jnp.where(low, got, 0.0)
    up = [(i, i + 1) for i in range(size - 1)]
    return lax.ppermute(last, "wav", up), lax.ppermute(first, "wav", [(j, i) for i, j in up])


def solution(mesh):
    return jax.shard_map(
        local,
        mesh=mesh,
        in_specs=(
            P(("grp", "fib"), "arm", None, None, "wav"),
            P(("grp", "fib"), "arm", None, None, "wav"),
            P(("grp", "fib"), None),
        ),
        out_specs=(
            P("arm", ("grp", "fib"), "wav"),
            P("arm", ("grp", "fib"), "wav"),
            P("arm", None, ("grp", "fib"), "wav"),
            P("arm", ("grp", "fib"), "wav"),
        ),
        check_vma=False,
    )
```
